8 devices in a mesh: dp: 1 (over z), tp: 8 (over y, x, core).
Axes of the slice: x: 2, y: 2, z: 1, core: 2. Of those that a mesh axis runs over, the one named last changes fastest.
Arguments:
- x_in: bfloat16 [3, 1536, 4096], P('dp', 'tp')
- positions: int32 [3, 1536], P('dp')
- prefix_len: int32 [3], P('dp')
- w_qkv: bfloat16 [4096, 12288], P(None, 'tp')
- b_qkv: bfloat16 [12288], P('tp')
- w_out: bfloat16 [4096, 4096], P('tp')
- b_out: bfloat16 [4096], replicated
- ln1_gain: bfloat16 [4096], replicated
- ln1_bias: bfloat16 [4096], replicated
- w_up: bfloat16 [4096, 28672], P(None, 'tp')
- b_up: bfloat16 [28672], P('tp')
- w_down: bfloat16 [14336, 4096], P('tp')
- b_down: bfloat16 [4096], replicated
- ln2_gain: bfloat16 [4096], replicated
- ln2_bias: bfloat16 [4096], replicated
Outputs:
- output: bfloat16 [3, 1536, 4096], P('dp', 'tp')
All inputs are finite; a program needn't handle non-finite values.
Results may differ from the reference program's by a relative error of at most 0.0193589.
Values are sent between devices in bfloat16 or wider.
A program may use at most 1 GiB of HBM per device.

```python
import math
import jax
import jax.numpy as jnp
from jax import lax

BATCH = 3
SEQ_LEN = 1536
HIDDEN = 4096
FFN_DIM = 14336
TP_GROUPS = 8
HEAD_DIM = 128
GLU_BLOCK = 128

NUM_HEADS = HIDDEN // HEAD_DIM
QUERY_BLOCK = min(SEQ_LEN, 256)
DEEPNORM_ALPHA = math.sqrt(2.0 * 70)
LN_EPS = 1e-5
ROPE_BASE = 10000.0


def setup_inputs(seed: int = 0, part: int = 0) -> dict:
    part_key = jax.random.fold_in(jax.random.key(seed), part)
    act_keys = jax.random.split(part_key, 3)
    weight_keys = jax.random.split(jax.random.key(seed + 1), 12)

    def normal_std(key_index, arr_shape, scale_std):
        return scale_std * jax.random.normal(weight_keys[key_index], arr_shape, jnp.float32)

    x_in = jax.random.normal(act_keys[0], (BATCH, SEQ_LEN, HIDDEN), jnp.float32)
    pos_steps = jax.random.randint(act_keys[1], (BATCH, SEQ_LEN), 0, 3)
    positions = jnp.cumsum(pos_steps, axis=1).astype(jnp.int32)
    prefix_len = jax.random.randint(act_keys[2], (BATCH,), 0, SEQ_LEN + 1).astype(jnp.int32)
    return {
        'x_in': x_in.astype(jnp.bfloat16),
        'positions': positions,
        'prefix_len': prefix_len,
        'w_qkv': normal_std(0, (HIDDEN, 3 * HIDDEN), 1.5 * HIDDEN ** -0.5).astype(jnp.bfloat16),
        'b_qkv': normal_std(1, (3 * HIDDEN,), 0.3).astype(jnp.bfloat16),
        'w_out': normal_std(2, (HIDDEN, HIDDEN), 2.0 * DEEPNORM_ALPHA * HIDDEN ** -0.5).astype(jnp.bfloat16),
        'b_out': normal_std(3, (HIDDEN,), 0.2 * DEEPNORM_ALPHA).astype(jnp.bfloat16),
        'ln1_gain': (1.0 + normal_std(4, (HIDDEN,), 0.2)).astype(jnp.bfloat16),
        'ln1_bias': normal_std(5, (HIDDEN,), 0.2).astype(jnp.bfloat16),
        'w_up': normal_std(6, (HIDDEN, 2 * FFN_DIM), HIDDEN ** -0.5).astype(jnp.bfloat16),
        'b_up': normal_std(7, (2 * FFN_DIM,), 0.3).astype(jnp.bfloat16),
        'w_down': normal_std(8, (FFN_DIM, HIDDEN), 1.5 * DEEPNORM_ALPHA * FFN_DIM ** -0.5).astype(jnp.bfloat16),
        'b_down': normal_std(9, (HIDDEN,), 0.2 * DEEPNORM_ALPHA).astype(jnp.bfloat16),
        'ln2_gain': (1.0 + normal_std(10, (HIDDEN,), 0.2)).astype(jnp.bfloat16),
        'ln2_bias': normal_std(11, (HIDDEN,), 0.2).astype(jnp.bfloat16),
    }


def layer_norm(resid, ln_gain, ln_bias):
    mean_val = jnp.mean(resid, axis=-1, keepdims=True)
    centered = resid - mean_val
    var_val = jnp.mean(centered * centered, axis=-1, keepdims=True)
    return centered * lax.rsqrt(var_val + LN_EPS) * ln_gain.astype(jnp.float32) + ln_bias.astype(jnp.float32)


def rope_tables(positions):
    inv_freq = ROPE_BASE ** (jnp.arange(HEAD_DIM // 2, dtype=jnp.float32) * (-2.0 / HEAD_DIM))
    angles = positions.astype(jnp.float32)[:, :, None] * inv_freq
    return jnp.cos(angles)[:, :, None, :], jnp.sin(angles)[:, :, None, :]


def apply_rope(head_vec, cos_t, sin_t):
    half_dim = HEAD_DIM // 2
    lower_half = head_vec[..., :half_dim].astype(jnp.float32)
    upper_half = head_vec[..., half_dim:].astype(jnp.float32)
    rotated = jnp.concatenate([lower_half * cos_t - upper_half * sin_t, upper_half * cos_t + lower_half * sin_t], axis=-1)
    return rotated.astype(jnp.bfloat16)


def group_sum(acts, weights):
    tokens = acts.shape[0]
    group_width = acts.shape[1] // TP_GROUPS
    act_groups = acts.reshape(tokens, TP_GROUPS, group_width).transpose(1, 0, 2)
    weight_groups = weights.reshape(TP_GROUPS, group_width, weights.shape[1])

    def add_group(running, group):
        act_blk, weight_blk = group
        group_prod = jnp.dot(act_blk, weight_blk, preferred_element_type=jnp.float32).astype(jnp.bfloat16)
        return running + group_prod.astype(jnp.float32), None

    start_sum = jnp.zeros((tokens, weights.shape[1]), jnp.float32)
    summed_out, _ = lax.scan(add_group, start_sum, (act_groups, weight_groups))
    return summed_out.astype(jnp.bfloat16)


def reference(x_in, positions, prefix_len, w_qkv, b_qkv, w_out, b_out, ln1_gain, ln1_bias, w_up, b_up, w_down, b_down, ln2_gain, ln2_bias):
    tokens = BATCH * SEQ_LEN
    x_flat = x_in.reshape(tokens, HIDDEN)
    qkv_all = jnp.dot(x_flat, w_qkv, preferred_element_type=jnp.float32) + b_qkv.astype(jnp.float32)
    qkv_all = qkv_all.astype(jnp.bfloat16).reshape(BATCH, SEQ_LEN, NUM_HEADS, 3, HEAD_DIM)
    cos_t, sin_t = rope_tables(positions)
    q_rot = apply_rope(qkv_all[:, :, :, 0], cos_t, sin_t).astype(jnp.float32)
    k_rot = apply_rope(qkv_all[:, :, :, 1], cos_t, sin_t).astype(jnp.float32)
    v_all = qkv_all[:, :, :, 2].astype(jnp.float32)
    key_idx = jnp.arange(SEQ_LEN)
    attn_scale = HEAD_DIM ** -0.5

    def attend(blk_idx):
        q_start = blk_idx * QUERY_BLOCK
        q_blk = lax.dynamic_slice_in_dim(q_rot, q_start, QUERY_BLOCK, axis=1)
        scores = jnp.einsum('bqnd,bknd->bnqk', q_blk, k_rot) * attn_scale
        q_idx = q_start + jnp.arange(QUERY_BLOCK)
        visible = (key_idx[None, None, :] < prefix_len[:, None, None]) | (key_idx[None, None, :] <= q_idx[None, :, None])
        scores = jnp.where(visible[:, None, :, :], scores, -1e30)
        attn_probs = jax.nn.softmax(scores, axis=-1).astype(jnp.bfloat16)
        return jnp.einsum('bnqk,bknd->bqnd', attn_probs.astype(jnp.float32), v_all).astype(jnp.bfloat16)

    context = lax.map(attend, jnp.arange(SEQ_LEN // QUERY_BLOCK))
    context = context.transpose(1, 0, 2, 3, 4).reshape(tokens, HIDDEN)
    attn_out = group_sum(context, w_out)
    resid1 = DEEPNORM_ALPHA * x_flat.astype(jnp.float32) + attn_out.astype(jnp.float32) + b_out.astype(jnp.float32)
    mid_norm = layer_norm(resid1, ln1_gain, ln1_bias).astype(jnp.bfloat16)
    up_proj = jnp.dot(mid_norm, w_up, preferred_element_type=jnp.float32) + b_up.astype(jnp.float32)
    up_proj = up_proj.astype(jnp.bfloat16).reshape(tokens, FFN_DIM // GLU_BLOCK, 2, GLU_BLOCK)
    value_part = up_proj[:, :, 0].astype(jnp.float32)
    gate_part = up_proj[:, :, 1].astype(jnp.float32)
    glu_out = (value_part * jax.nn.gelu(gate_part, approximate=True)).astype(jnp.bfloat16).reshape(tokens, FFN_DIM)
    ffn_out = group_sum(glu_out, w_down)
    resid2 = DEEPNORM_ALPHA * mid_norm.astype(jnp.float32) + ffn_out.astype(jnp.float32) + b_down.astype(jnp.float32)
    y_out = layer_norm(resid2, ln2_gain, ln2_bias).astype(jnp.bfloat16)
    return y_out.reshape(BATCH, SEQ_LEN, HIDDEN)
```

```python
import functools
import math
import jax
import jax.numpy as jnp
from jax import lax
from jax.experimental import pallas as pl
from jax.experimental.pallas import tpu as pltpu
from jax.sharding import PartitionSpec as P

HEAD_DIM = 128
GLU_BLOCK = 128
DEEPNORM_ALPHA = math.sqrt(2.0 * 70)
LN_EPS = 1e-5
ROPE_BASE = 10000.0
F32 = jnp.float32
BF16 = jnp.bfloat16


def layer_norm(resid, ln_gain, ln_bias):
    mean_val = jnp.mean(resid, axis=-1, keepdims=True)
    centered = resid - mean_val
    var_val = jnp.mean(centered * centered, axis=-1, keepdims=True)
    return centered * lax.rsqrt(var_val + LN_EPS) * ln_gain.astype(F32) + ln_bias.astype(F32)


def rope_tables(positions):
    inv_freq = ROPE_BASE ** (jnp.arange(HEAD_DIM // 2, dtype=F32) * (-2.0 / HEAD_DIM))
    angles = positions.astype(F32)[:, :, None] * inv_freq
    cos_t, sin_t = jnp.cos(angles), jnp.sin(angles)
    return jnp.concatenate([cos_t, cos_t], axis=-1), jnp.concatenate([-sin_t, sin_t], axis=-1)


def rotate(vec, cos_t, sin_t):
    wide = vec.astype(F32)
    return (wide * cos_t + pltpu.roll(wide, HEAD_DIM // 2, 1) * sin_t).astype(BF16)


def attn_kernel(rows, seq_len, key_block, info, qkv_ref, cos_ref, sin_ref, mine_ref, other_ref, k_ref):
    q_blk = pl.program_id(1)
    prefix, core = info[0], info[1]
    q_rows = 2 * rows

    @pl.when(q_blk == 0)
    def _():
        k_ref[...] = rotate(qkv_ref[:, HEAD_DIM:2 * HEAD_DIM], cos_ref[...], sin_ref[...])

    q_start = pl.multiple_of(q_blk * q_rows, q_rows)
    limit = jnp.maximum(prefix, q_start + q_rows)
    need = lax.div(limit + (key_block - 1), key_block)
    exp_scale = HEAD_DIM ** -0.5 * math.log2(math.e)

    def half(which, keys):
        at = pl.multiple_of(q_start + which * rows, rows)
        here = pl.ds(at, rows)
        q_rot = rotate(qkv_ref[here, 0:HEAD_DIM], cos_ref[here, :], sin_ref[here, :])
        scores = lax.dot_general(q_rot, k_ref[0:keys, :], (((1,), (1,)), ((), ())), preferred_element_type=F32)
        row_last = jnp.maximum(lax.broadcasted_iota(jnp.int32, (rows, 1), 0) + at, prefix - 1)
        key_idx = lax.broadcasted_iota(jnp.int32, (rows, keys), 1)
        scores = jnp.where(key_idx <= row_last, scores, -1e30)
        top = jnp.max(scores, axis=-1, keepdims=True)
        probs = jnp.exp2(scores * exp_scale - top * exp_scale)
        inv_sum = 1.0 / jnp.sum(probs, axis=-1, keepdims=True)
        probs = (probs * inv_sum).astype(BF16)
        v_all = qkv_ref[0:keys, 2 * HEAD_DIM:3 * HEAD_DIM]
        return jnp.dot(probs, v_all, preferred_element_type=F32)

    for blocks in range(1, seq_len // key_block + 1):
        @pl.when(need == blocks)
        def _(keys=blocks * key_block):
            first, second = half(0, keys), half(1, keys)
            mine_ref[...] = jnp.where(core == 0, first, second).astype(BF16)
            other_ref[...] = jnp.where(core == 0, second, first).astype(BF16)


def attention(info, qkv, cos_t, sin_t, rows):
    seq_len, width = qkv.shape
    heads = width // (3 * HEAD_DIM)
    half_len = seq_len // 2
    key_block = 2 * rows
    out = jax.ShapeDtypeStruct((half_len, heads * HEAD_DIM), BF16)
    out_spec = pl.BlockSpec((rows, HEAD_DIM), lambda h, i, info: (i, h))
    return pl.pallas_call(
        functools.partial(attn_kernel, rows, seq_len, key_block),
        out_shape=(out, out),
        grid_spec=pltpu.PrefetchScalarGridSpec(
            num_scalar_prefetch=1,
            grid=(heads, seq_len // (2 * rows)),
            in_specs=[
                pl.BlockSpec((seq_len, 3 * HEAD_DIM), lambda h, i, info: (0, h)),
                pl.BlockSpec((seq_len, HEAD_DIM), lambda h, i, info: (0, 0)),
                pl.BlockSpec((seq_len, HEAD_DIM), lambda h, i, info: (0, 0)),
            ],
            out_specs=[out_spec, out_spec],
            scratch_shapes=[pltpu.VMEM((seq_len, HEAD_DIM), BF16)],
        ),
        compiler_params=pltpu.CompilerParams(vmem_limit_bytes=40 << 20),
        cost_estimate=pl.CostEstimate(flops=24 * 10 ** 9, bytes_accessed=12 << 20, transcendentals=heads * seq_len * seq_len),
        name='attention',
    )(info, qkv, cos_t, sin_t)


def split_kernel(w_ref, value_ref, gate_ref):
    value_ref[...] = w_ref[:, :GLU_BLOCK]
    gate_ref[...] = w_ref[:, GLU_BLOCK:]


def split_pairs(w_up):
    depth, width = w_up.shape
    out = jax.ShapeDtypeStruct((depth, width // 2), w_up.dtype)
    spec = pl.BlockSpec((depth, GLU_BLOCK), lambda j: (0, j))
    return pl.pallas_call(
        split_kernel,
        out_shape=(out, out),
        grid=(width // (2 * GLU_BLOCK),),
        in_specs=[pl.BlockSpec((depth, 2 * GLU_BLOCK), lambda j: (0, j))],
        out_specs=[spec, spec],
        compiler_params=pltpu.CompilerParams(vmem_limit_bytes=24 << 20),
        cost_estimate=pl.CostEstimate(flops=18 * 10 ** 9, bytes_accessed=4 * depth * width, transcendentals=0),
        name='split_pairs',
    )(w_up)


def mm(lhs, rhs):
    return jnp.dot(lhs, rhs, preferred_element_type=F32)


def glu(rows, w_pair, b_pair):
    value = (mm(rows, w_pair[0]) + b_pair[0].astype(F32)).astype(BF16)
    gate = (mm(rows, w_pair[1]) + b_pair[1].astype(F32)).astype(BF16)
    return (value.astype(F32) * jax.nn.gelu(gate.astype(F32), approximate=True)).astype(BF16)


def two_part_sum(lhs_pair, rhs_pair):
    first = mm(lhs_pair[0], rhs_pair[0]).astype(BF16)
    second = mm(lhs_pair[1], rhs_pair[1]).astype(BF16)
    return (first.astype(F32) + second.astype(F32)).astype(BF16)


def solution(mesh):
    tp = mesh.shape['tp']
    swap = [(i, i ^ 1) for i in range(tp)]
    same_core = [list(range(0, tp, 2)), list(range(1, tp, 2))]

    def partner(val):
        return lax.ppermute(val, 'tp', swap)

    def local_layer(x_loc, positions, prefix_len, w_qkv, b_qkv, w_out, b_out, ln1_gain, ln1_bias, w_up, b_up, w_down, b_down, ln2_gain, ln2_bias):
        batch_size, seq_loc, model_dim = x_loc.shape
        core = lax.axis_index('tp') % 2
        gathered = [lax.all_gather(x_loc[b], 'tp', axis=0, tiled=True) for b in range(batch_size)]
        cos_t, sin_t = rope_tables(positions)
        w_pair = split_pairs(w_up)
        b_rows = b_up.reshape(-1, 2, GLU_BLOCK)
        b_pair = (b_rows[:, 0].reshape(-1), b_rows[:, 1].reshape(-1))
        outs_w = (w_out, partner(w_out))
        down_w = (w_down, partner(w_down))
        up_w = (w_pair, (partner(w_pair[0]), partner(w_pair[1])))
        b_other = partner(jnp.stack(b_pair))
        up_b = (b_pair, (b_other[0], b_other[1]))

        attn_loc = []
        for b in range(batch_size):
            qkv = (mm(gathered[b], w_qkv) + b_qkv.astype(F32)).astype(BF16)
            info = jnp.stack([prefix_len[b], core]).astype(jnp.int32)
            mine, other = attention(info, qkv, cos_t[b], sin_t[b], seq_loc)
            part = two_part_sum((mine, partner(other)), outs_w)
            attn_loc.append(lax.psum_scatter(part, 'tp', scatter_dimension=0, axis_index_groups=same_core, tiled=True))

        mids, fulls = [], []
        for b in range(batch_size):
            resid1 = DEEPNORM_ALPHA * x_loc[b].astype(F32) + attn_loc[b].astype(F32) + b_out.astype(F32)
            mids.append(layer_norm(resid1, ln1_gain, ln1_bias).astype(BF16))
            fulls.append(lax.all_gather(mids[b], 'tp', axis=0, axis_index_groups=same_core, tiled=True))

        outs = []
        for b in range(batch_size):
            acts = tuple(glu(fulls[b], up_w[i], up_b[i]) for i in range(2))
            part = two_part_sum(acts, down_w)
            ffn_loc = lax.psum_scatter(part, 'tp', scatter_dimension=0, axis_index_groups=same_core, tiled=True)
            resid2 = DEEPNORM_ALPHA * mids[b].astype(F32) + ffn_loc.astype(F32) + b_down.astype(F32)
            outs.append(layer_norm(resid2, ln2_gain, ln2_bias).astype(BF16))
        return jnp.stack(outs)

    in_specs = (P('dp', 'tp', None), P('dp', None), P('dp'), P(None, 'tp'), P('tp'), P('tp', None), P(), P(), P(), P(None, 'tp'), P('tp'), P('tp', None), P(), P(), P())
    return jax.shard_map(local_layer, mesh=mesh, in_specs=in_specs, out_specs=P('dp', 'tp', None), check_vma=False)
```

```python
import functools
import math
import jax
import jax.numpy as jnp
from jax import lax
from jax.experimental import pallas as pl
from jax.experimental.pallas import tpu as pltpu
from jax.sharding import PartitionSpec as P

HEAD_DIM = 128
GLU_BLOCK = 128
DEEPNORM_ALPHA = math.sqrt(2.0 * 70)
LN_EPS = 1e-5
ROPE_BASE = 10000.0
F32 = jnp.float32
BF16 = jnp.bfloat16


def layer_norm(resid, ln_gain, ln_bias):
    mean_val = jnp.mean(resid, axis=-1, keepdims=True)
    centered = resid - mean_val
    var_val = jnp.mean(centered * centered, axis=-1, keepdims=True)
    return centered * lax.rsqrt(var_val + LN_EPS) * ln_gain.astype(F32) + ln_bias.astype(F32)


def rope_tables(positions):
    inv_freq = ROPE_BASE ** (jnp.arange(HEAD_DIM // 2, dtype=F32) * (-2.0 / HEAD_DIM))
    angles = positions.astype(F32)[:, :, None] * inv_freq
    cos_t, sin_t = jnp.cos(angles), jnp.sin(angles)
    return jnp.concatenate([cos_t, cos_t], axis=-1), jnp.concatenate([-sin_t, sin_t], axis=-1)


def rotate(vec, cos_t, sin_t):
    wide = vec.astype(F32)
    return (wide * cos_t + pltpu.roll(wide, HEAD_DIM // 2, 1) * sin_t).astype(BF16)


def attn_kernel(rows, seq_len, key_block, info, qkv_ref, cos_ref, sin_ref, mine_ref, other_ref, k_ref):
    q_blk = pl.program_id(1)
    prefix, core = info[0], info[1]
    q_rows = 2 * rows

    @pl.when(q_blk == 0)
    def _():
        k_ref[...] = rotate(qkv_ref[:, HEAD_DIM:2 * HEAD_DIM], cos_ref[...], sin_ref[...])

    q_start = pl.multiple_of(q_blk * q_rows, q_rows)
    limit = jnp.maximum(prefix, q_start + q_rows)
    need = lax.div(limit + (key_block - 1), key_block)
    exp_scale = HEAD_DIM ** -0.5 * math.log2(math.e)

    def half(which, keys):
        at = pl.multiple_of(q_start + which * rows, rows)
        here = pl.ds(at, rows)
        q_rot = rotate(qkv_ref[here, 0:HEAD_DIM], cos_ref[here, :], sin_ref[here, :])
        scores = lax.dot_general(q_rot, k_ref[0:keys, :], (((1,), (1,)), ((), ())), preferred_element_type=F32)
        row_last = jnp.maximum(lax.broadcasted_iota(jnp.int32, (rows, 1), 0) + at, prefix - 1)
        key_idx = lax.broadcasted_iota(jnp.int32, (rows, keys), 1)
        scores = jnp.where(key_idx <= row_last, scores, -1e30)
        top = jnp.max(scores, axis=-1, keepdims=True)
        probs = jnp.exp2(scores * exp_scale - top * exp_scale)
        inv_sum = 1.0 / jnp.sum(probs, axis=-1, keepdims=True)
        probs = (probs * inv_sum).astype(BF16)
        v_all = qkv_ref[0:keys, 2 * HEAD_DIM:3 * HEAD_DIM]
        return jnp.dot(probs, v_all, preferred_element_type=F32)

    for blocks in range(1, seq_len // key_block + 1):
        @pl.when(need == blocks)
        def _(keys=blocks * key_block):
            first, second = half(0, keys), half(1, keys)
            mine_ref[...] = jnp.where(core == 0, first, second).astype(BF16)
            other_ref[...] = jnp.where(core == 0, second, first).astype(BF16)


def attention(info, qkv, cos_t, sin_t, rows):
    seq_len, width = qkv.shape
    heads = width // (3 * HEAD_DIM)
    half_len = seq_len // 2
    key_block = 2 * rows
    out = jax.ShapeDtypeStruct((half_len, heads * HEAD_DIM), BF16)
    out_spec = pl.BlockSpec((rows, HEAD_DIM), lambda h, i, info: (i, h))
    return pl.pallas_call(
        functools.partial(attn_kernel, rows, seq_len, key_block),
        out_shape=(out, out),
        grid_spec=pltpu.PrefetchScalarGridSpec(
            num_scalar_prefetch=1,
            grid=(heads, seq_len // (2 * rows)),
            in_specs=[
                pl.BlockSpec((seq_len, 3 * HEAD_DIM), lambda h, i, info: (0, h)),
                pl.BlockSpec((seq_len, HEAD_DIM), lambda h, i, info: (0, 0)),
                pl.BlockSpec((seq_len, HEAD_DIM), lambda h, i, info: (0, 0)),
            ],
            out_specs=[out_spec, out_spec],
            scratch_shapes=[pltpu.VMEM((seq_len, HEAD_DIM), BF16)],
        ),
        compiler_params=pltpu.CompilerParams(vmem_limit_bytes=40 << 20),
        cost_estimate=pl.CostEstimate(flops=24 * 10 ** 9, bytes_accessed=12 << 20, transcendentals=heads * seq_len * seq_len),
        name='attention',
    )(info, qkv, cos_t, sin_t)


def norm_kernel(x_ref, part_ref, bias_ref, gain_ref, shift_ref, *out_refs):
    resid = DEEPNORM_ALPHA * x_ref[...].astype(F32) + part_ref[...].astype(F32) + bias_ref[...].astype(F32)
    out_refs[-1][...] = layer_norm(resid, gain_ref[...], shift_ref[...]).astype(BF16)


def norm_rows(x_rows, x_at, part, bias, gain, shift, out_rows=None, out_at=None, into=None):
    rows, width = part.shape
    step = 64
    spec = pl.BlockSpec((step, width), lambda i: (i, 0))
    vec = pl.BlockSpec((1, width), lambda i: (0, 0))
    x_spec = spec if x_at is None else pl.BlockSpec((None, step, width), lambda i: (x_at, i, 0))
    args = [x_rows, part, bias.reshape(1, -1), gain.reshape(1, -1), shift.reshape(1, -1)]
    in_specs = [x_spec, spec, vec, vec, vec]
    alias = {}
    if out_rows is None:
        out, out_spec = jax.ShapeDtypeStruct((rows, width), BF16), spec
    else:
        out = jax.ShapeDtypeStruct((out_rows, rows, width), BF16)
        out_spec = pl.BlockSpec((None, step, width), lambda i: (out_at, i, 0))
    if into is not None:
        args.append(into)
        in_specs.append(pl.BlockSpec(memory_space=pl.ANY))
        alias = {5: 0}
    return pl.pallas_call(
        norm_kernel,
        out_shape=out,
        grid=(rows // step,),
        in_specs=in_specs,
        out_specs=out_spec,
        input_output_aliases=alias,
        compiler_params=pltpu.CompilerParams(vmem_limit_bytes=24 << 20),
        cost_estimate=pl.CostEstimate(flops=3 * 10 ** 9, bytes_accessed=6 * rows * width, transcendentals=0),
        name='norm_rows',
    )(*args)


UP_TILE = 512
UP_ROWS = 384


def up_kernel(tiles, own_rows, info, own_ref, x_ref, y_ref, far_a_ref, far_b_ref, w_own, w_other, b_ref, m_ref, h_buf, w_buf, h_sem, w_sem):
    step = pl.program_id(0)
    chip = info[2]
    half = own_rows // 2

    def weight_copy(at, start):
        slot = lax.rem(at, 2)

        def go(src, tile):
            cols = pl.ds(pl.multiple_of(tile * UP_TILE, UP_TILE), UP_TILE)
            copy = pltpu.make_async_copy(src.at[:, cols], w_buf.at[slot], w_sem.at[slot])
            copy.start() if start else copy.wait()

        if not start:
            go(w_own, 0)
            return

        @pl.when(at < tiles)
        def _():
            go(w_own, at)

        @pl.when(at >= tiles)
        def _():
            go(w_other, at - tiles)

    def row_copies():
        parts = ((own_ref, 0, 0, own_rows), (x_ref, 1, 0, own_rows), (y_ref, 2, 0, own_rows), (far_a_ref, 3, 0, half), (far_b_ref, 3, half, half))
        for k, (src, flip, shift, size) in enumerate(parts):
            at = pl.multiple_of(jnp.bitwise_xor(chip, flip) * own_rows + shift, half)
            yield pltpu.make_async_copy(src, h_buf.at[pl.ds(at, size), :], h_sem.at[k])

    @pl.when(step == 0)
    def _():
        weight_copy(step, True)
        for copy in row_copies():
            copy.start()

    @pl.when(step + 1 < 2 * tiles)
    def _():
        weight_copy(step + 1, True)

    weight_copy(step, False)

    @pl.when(step == 0)
    def _():
        for copy in row_copies():
            copy.wait()

    slot = lax.rem(step, 2)
    bias = b_ref[...].astype(F32)

    @pl.loop(0, h_buf.shape[0] // UP_ROWS)
    def _(block):
        here = pl.ds(pl.multiple_of(block * UP_ROWS, UP_ROWS), UP_ROWS)
        up = jnp.dot(h_buf[here, :], w_buf[slot], preferred_element_type=F32)
        up = (up + bias).astype(BF16).astype(F32)
        for pair in range(UP_TILE // (2 * GLU_BLOCK)):
            base = 2 * GLU_BLOCK * pair
            value, gate = up[:, base:base + GLU_BLOCK], up[:, base + GLU_BLOCK:base + 2 * GLU_BLOCK]
            m_ref[here, GLU_BLOCK * pair:GLU_BLOCK * (pair + 1)] = (value * jax.nn.gelu(gate, approximate=True)).astype(BF16)


def up_glu(info, row_parts, w_own, w_other, b_all):
    own_rows, depth = row_parts[0].shape
    rows = 4 * own_rows
    width = w_own.shape[1]
    tiles = width // UP_TILE
    hbm = pl.BlockSpec(memory_space=pl.ANY)
    return pl.pallas_call(
        functools.partial(up_kernel, tiles, own_rows),
        out_shape=jax.ShapeDtypeStruct((rows, width), BF16),
        grid_spec=pltpu.PrefetchScalarGridSpec(
            num_scalar_prefetch=1,
            grid=(2 * tiles,),
            in_specs=[hbm] * 7 + [pl.BlockSpec((1, UP_TILE), lambda j, info: (0, j))],
            out_specs=pl.BlockSpec((rows, UP_TILE // 2), lambda j, info: (0, j)),
            scratch_shapes=[
                pltpu.VMEM((rows, depth), BF16),
                pltpu.VMEM((2, depth, UP_TILE), BF16),
                pltpu.SemaphoreType.DMA((5,)),
                pltpu.SemaphoreType.DMA((2,)),
            ],
        ),
        compiler_params=pltpu.CompilerParams(vmem_limit_bytes=32 << 20),
        cost_estimate=pl.CostEstimate(flops=4 * rows * depth * width, bytes_accessed=4 * depth * width, transcendentals=rows * width),
        name='up_glu',
    )(info, *row_parts, w_own, w_other, b_all)


def pair_kernel(a_ref, b_ref, wa_ref, wb_ref, out_ref):
    first = jnp.dot(a_ref[...], wa_ref[...], preferred_element_type=F32).astype(BF16)
    second = jnp.dot(b_ref[...], wb_ref[...], preferred_element_type=F32).astype(BF16)
    out_ref[...] = (first.astype(F32) + second.astype(F32)).astype(BF16)


def pair_product(lhs, w_own, w_other, tile, row_tile):
    depth, width = w_own.shape
    rows = lhs[0].shape[0]
    second = 1 if lhs[0] is lhs[1] else 0
    w_spec = pl.BlockSpec((depth, tile), lambda j, i: (0, j))
    return pl.pallas_call(
        pair_kernel,
        out_shape=jax.ShapeDtypeStruct((rows, width), BF16),
        grid=(width // tile, rows // row_tile),
        in_specs=[
            pl.BlockSpec((row_tile, depth), lambda j, i: (i, 0)),
            pl.BlockSpec((row_tile, depth), lambda j, i: (i, second)),
            w_spec,
            w_spec,
        ],
        out_specs=pl.BlockSpec((row_tile, tile), lambda j, i: (i, j)),
        compiler_params=pltpu.CompilerParams(vmem_limit_bytes=32 << 20),
        cost_estimate=pl.CostEstimate(flops=4 * rows * depth * width, bytes_accessed=4 * depth * width, transcendentals=0),
    )(*lhs, w_own, w_other)


def mm(lhs, rhs):
    return jnp.dot(lhs, rhs, preferred_element_type=F32)


def solution(mesh):
    tp = mesh.shape['tp']
    same_core = [list(range(0, tp, 2)), list(range(1, tp, 2))]

    def from_peer(val, flip):
        return lax.ppermute(val, 'tp', [(i, i ^ flip) for i in range(tp)])

    def layer(x_loc, positions, prefix_len, w_qkv, b_qkv, w_out, b_out, ln1_gain, ln1_bias, w_up, b_up, w_down, b_down, ln2_gain, ln2_bias):
        batch_size, seq_loc, _ = x_loc.shape
        me = lax.axis_index('tp')
        half = seq_loc // 2
        gathered = [lax.all_gather(x_loc[b], 'tp', axis=0, tiled=True) for b in range(batch_size)]
        cos_t, sin_t = rope_tables(positions)
        infos = [jnp.stack([prefix_len[b], me % 2, me // 2]).astype(jnp.int32) for b in range(batch_size)]
        out_other, up_other, down_other = from_peer(w_out, 1), from_peer(w_up, 1), from_peer(w_down, 1)
        b_all = jnp.concatenate([b_up, from_peer(b_up, 1)]).reshape(1, -1)

        attn_loc = []
        for b in range(batch_size):
            if b == batch_size - 1:
                gathered[b], up_other, down_other = lax.optimization_barrier((gathered[b], up_other, down_other))
            qkv = (mm(gathered[b], w_qkv) + b_qkv.astype(F32)).astype(BF16)
            mine, other = attention(infos[b], qkv, cos_t[b], sin_t[b], seq_loc)
            part = pair_product((mine, from_peer(other, 1)), w_out, out_other, 1024, 768)
            attn_loc.append(lax.psum_scatter(part, 'tp', scatter_dimension=0, axis_index_groups=same_core, tiled=True))

        def first_norm(b):
            return norm_rows(x_loc, b, attn_loc[b], b_out, ln1_gain, ln1_bias)

        def near_rows(mid):
            return from_peer(mid, 2), from_peer(mid, 4)

        def far_rows(near):
            return from_peer(near[1][:half], 2), from_peer(near[0][half:], 4)

        result = None
        mid = first_norm(0)
        near = near_rows(mid)
        far = far_rows(near)
        for b in range(batch_size):
            parts = (mid, *near, *far)
            last = b == batch_size - 1
            if not last:
                parts, next_mid = lax.optimization_barrier((parts, first_norm(b + 1)))
                next_near = near_rows(next_mid)
            acts = up_glu(infos[b], parts, w_up, up_other, b_all)
            if not last:
                acts, next_near = lax.optimization_barrier((acts, next_near))
                next_far = far_rows(next_near)
            part = pair_product((acts, acts), w_down, down_other, 512, 768)
            ffn_loc = lax.psum_scatter(part, 'tp', scatter_dimension=0, axis_index_groups=same_core, tiled=True)
            result = norm_rows(mid, None, ffn_loc, b_down, ln2_gain, ln2_bias, batch_size, b, result)
            if not last:
                mid, near, far = next_mid, next_near, next_far
        return result

    in_specs = (P('dp', 'tp', None), P('dp', None), P('dp'), P(None, 'tp'), P('tp'), P('tp', None), P(), P(), P(), P(None, 'tp'), P('tp'), P('tp', None), P(), P(), P())
    return jax.shard_map(layer, mesh=mesh, in_specs=in_specs, out_specs=P('dp', 'tp', None), check_vma=False)
```

```python
import functools
import math
import jax
import jax.numpy as jnp
from jax import lax
from jax.experimental import pallas as pl
from jax.experimental.pallas import tpu as pltpu
from jax.sharding import PartitionSpec as P


HEAD_DIM = 128
GLU_BLOCK = 128
DEEPNORM_ALPHA = math.sqrt(2.0 * 70)
LN_EPS = 1e-5
ROPE_BASE = 10000.0
VMEM_LIMIT = 60 << 20
F32 = jnp.float32
BF16 = jnp.bfloat16


def layer_norm(resid, ln_gain, ln_bias):
    mean_val = jnp.mean(resid, axis=-1, keepdims=True)
    centered = resid - mean_val
    var_val = jnp.mean(centered * centered, axis=-1, keepdims=True)
    return centered * lax.rsqrt(var_val + LN_EPS) * ln_gain.astype(F32) + ln_bias.astype(F32)


def rope_tables(positions):
    inv_freq = ROPE_BASE ** (jnp.arange(HEAD_DIM // 2, dtype=F32) * (-2.0 / HEAD_DIM))
    angles = positions.astype(F32)[:, :, None] * inv_freq
    cos_t, sin_t = jnp.cos(angles), jnp.sin(angles)
    return jnp.concatenate([cos_t, cos_t], axis=-1), jnp.concatenate([-sin_t, sin_t], axis=-1)


def rotate(vec, cos_t, sin_t):
    wide = vec.astype(F32)
    return (wide * cos_t + pltpu.roll(wide, HEAD_DIM // 2, 1) * sin_t).astype(BF16)


def attn_kernel(rows, seq_len, key_block, info, qkv_ref, cos_ref, sin_ref, mine_ref, other_ref, k_ref):
    q_blk = pl.program_id(1)
    prefix, core = info[0], info[1]
    q_rows = 2 * rows

    @pl.when(q_blk == 0)
    def _():
        k_ref[...] = rotate(qkv_ref[:, HEAD_DIM:2 * HEAD_DIM], cos_ref[...], sin_ref[...])

    q_start = pl.multiple_of(q_blk * q_rows, q_rows)
    limit = jnp.maximum(prefix, q_start + q_rows)
    need = lax.div(limit + (key_block - 1), key_block)
    exp_scale = HEAD_DIM ** -0.5 * math.log2(math.e)

    def half(which, keys):
        at = pl.multiple_of(q_start + which * rows, rows)
        here = pl.ds(at, rows)
        q_rot = rotate(qkv_ref[here, 0:HEAD_DIM], cos_ref[here, :], sin_ref[here, :])
        scores = lax.dot_general(q_rot, k_ref[0:keys, :], (((1,), (1,)), ((), ())), preferred_element_type=F32)
        row_last = jnp.maximum(lax.broadcasted_iota(jnp.int32, (rows, 1), 0) + at, prefix - 1)
        key_idx = lax.broadcasted_iota(jnp.int32, (rows, keys), 1)
        scores = jnp.where(key_idx <= row_last, scores, -1e30)
        top = jnp.max(scores, axis=-1, keepdims=True)
        probs = jnp.exp2(scores * exp_scale - top * exp_scale)
        inv_sum = 1.0 / jnp.sum(probs, axis=-1, keepdims=True)
        probs = (probs * inv_sum).astype(BF16)
        v_all = qkv_ref[0:keys, 2 * HEAD_DIM:3 * HEAD_DIM]
        return jnp.dot(probs, v_all, preferred_element_type=F32)

    for blocks in range(1, seq_len // key_block + 1):
        @pl.when(need == blocks)
        def _(keys=blocks * key_block):
            first, second = half(0, keys), half(1, keys)
            mine_ref[...] = jnp.where(core == 0, first, second).astype(BF16)
            other_ref[...] = jnp.where(core == 0, second, first).astype(BF16)


def attention(info, qkv, cos_t, sin_t, rows):
    seq_len, width = qkv.shape
    heads = width // (3 * HEAD_DIM)
    half_len = seq_len // 2
    key_block = 2 * rows
    out = jax.ShapeDtypeStruct((half_len, heads * HEAD_DIM), BF16)
    out_spec = pl.BlockSpec((rows, HEAD_DIM), lambda h, i, info: (i, h))
    return pl.pallas_call(
        functools.partial(attn_kernel, rows, seq_len, key_block),
        out_shape=(out, out),
        grid_spec=pltpu.PrefetchScalarGridSpec(
            num_scalar_prefetch=1,
            grid=(heads, seq_len // (2 * rows)),
            in_specs=[
                pl.BlockSpec((seq_len, 3 * HEAD_DIM), lambda h, i, info: (0, h)),
                pl.BlockSpec((seq_len, HEAD_DIM), lambda h, i, info: (0, 0)),
                pl.BlockSpec((seq_len, HEAD_DIM), lambda h, i, info: (0, 0)),
            ],
            out_specs=[out_spec, out_spec],
            scratch_shapes=[pltpu.VMEM((seq_len, HEAD_DIM), BF16)],
        ),
        compiler_params=pltpu.CompilerParams(vmem_limit_bytes=VMEM_LIMIT),
        cost_estimate=pl.CostEstimate(flops=24 * 10 ** 9, bytes_accessed=12 << 20, transcendentals=heads * seq_len * seq_len),
        name='attention',
    )(info, qkv, cos_t, sin_t)


def norm_kernel(x_ref, part_ref, bias_ref, gain_ref, shift_ref, *out_refs):
    resid = DEEPNORM_ALPHA * x_ref[...].astype(F32) + part_ref[...].astype(F32) + bias_ref[...].astype(F32)
    out_refs[-1][...] = layer_norm(resid, gain_ref[...], shift_ref[...]).astype(BF16)


def norm_rows(x_rows, x_at, part, bias, gain, shift, out_rows=None, out_at=None, into=None):
    rows, width = part.shape
    step = 64
    spec = pl.BlockSpec((step, width), lambda i: (i, 0))
    vec = pl.BlockSpec((1, width), lambda i: (0, 0))
    x_spec = spec if x_at is None else pl.BlockSpec((None, step, width), lambda i: (x_at, i, 0))
    args = [x_rows, part, bias.reshape(1, -1), gain.reshape(1, -1), shift.reshape(1, -1)]
    in_specs = [x_spec, spec, vec, vec, vec]
    alias = {}
    if out_rows is None:
        out, out_spec = jax.ShapeDtypeStruct((rows, width), BF16), spec
    else:
        out = jax.ShapeDtypeStruct((out_rows, rows, width), BF16)
        out_spec = pl.BlockSpec((None, step, width), lambda i: (out_at, i, 0))
    if into is not None:
        args.append(into)
        in_specs.append(pl.BlockSpec(memory_space=pl.ANY))
        alias = {5: 0}
    return pl.pallas_call(
        norm_kernel,
        out_shape=out,
        grid=(rows // step,),
        in_specs=in_specs,
        out_specs=out_spec,
        input_output_aliases=alias,
        compiler_params=pltpu.CompilerParams(vmem_limit_bytes=VMEM_LIMIT),
        cost_estimate=pl.CostEstimate(flops=3 * 10 ** 9, bytes_accessed=6 * rows * width, transcendentals=0),
        name='norm_rows',
    )(*args)


QKV_TILE = 512
ROW_BLOCK = 384


def qkv_kernel(pieces, info, *refs):
    piece_refs, (w_ref, b_ref, out_ref, x_buf, x_sem) = refs[:len(pieces)], refs[len(pieces):]
    first = pl.program_id(0) == 0
    in_order = pieces[0] is None
    bias = b_ref[...].astype(F32)

    def piece_copy(k):
        if in_order:
            return pltpu.make_async_copy(
                piece_refs[0].at[pl.ds(k * ROW_BLOCK, ROW_BLOCK), :], x_buf.at[pl.ds(k * ROW_BLOCK, ROW_BLOCK), :], x_sem.at[k])
        flip, other, shift, size, whole = pieces[k]
        device = 2 * jnp.bitwise_xor(info[2], flip) + jnp.bitwise_xor(info[1], other)
        at = pl.multiple_of(device * whole + shift, size)
        return pltpu.make_async_copy(piece_refs[k], x_buf.at[pl.ds(at, size), :], x_sem.at[k])

    blocks = x_buf.shape[0] // ROW_BLOCK
    copies = blocks if in_order else len(pieces)

    @pl.when(first)
    def _():
        for k in range(copies):
            piece_copy(k).start()
        if not in_order:
            for k in range(copies):
                piece_copy(k).wait()

    @pl.loop(0, blocks)
    def _(block):
        here = pl.ds(pl.multiple_of(block * ROW_BLOCK, ROW_BLOCK), ROW_BLOCK)
        if in_order:
            @pl.when(first)
            def _():
                pltpu.make_async_copy(piece_refs[0].at[here, :], x_buf.at[here, :], x_sem.at[block]).wait()
        out_ref[here, :] = (jnp.dot(x_buf[here, :], w_ref[...], preferred_element_type=F32) + bias).astype(BF16)


def qkv_product(info, row_refs, pieces, w_qkv, b_qkv):
    depth, width = w_qkv.shape
    rows = sum(r.shape[0] for r in row_refs)
    hbm = pl.BlockSpec(memory_space=pl.ANY)
    return pl.pallas_call(
        functools.partial(qkv_kernel, pieces),
        out_shape=jax.ShapeDtypeStruct((rows, width), BF16),
        grid_spec=pltpu.PrefetchScalarGridSpec(
            num_scalar_prefetch=1,
            grid=(width // QKV_TILE,),
            in_specs=[hbm] * len(row_refs) + [
                pl.BlockSpec((depth, QKV_TILE), lambda j, info: (0, j)),
                pl.BlockSpec((1, QKV_TILE), lambda j, info: (0, j)),
            ],
            out_specs=pl.BlockSpec((rows, QKV_TILE), lambda j, info: (0, j)),
            scratch_shapes=[
                pltpu.VMEM((rows, depth), BF16),
                pltpu.SemaphoreType.DMA((max(len(pieces), rows // ROW_BLOCK),)),
            ],
        ),
        compiler_params=pltpu.CompilerParams(vmem_limit_bytes=VMEM_LIMIT),
        cost_estimate=pl.CostEstimate(flops=2 * rows * depth * width, bytes_accessed=2 * depth * (rows + width), transcendentals=0),
        name='qkv',
    )(info, *row_refs, w_qkv, b_qkv.reshape(1, -1))


UP_TILE = 512
UP_ROWS = 384


def up_kernel(tiles, own_rows, info, own_ref, x_ref, y_ref, far_a_ref, far_b_ref, w_own, w_other, b_ref, m_ref, h_buf, w_buf, h_sem, w_sem):
    step = pl.program_id(0)
    chip = info[2]
    half = own_rows // 2

    def weight_copy(at, start):
        slot = lax.rem(at, 2)

        def go(src, tile):
            cols = pl.ds(pl.multiple_of(tile * UP_TILE, UP_TILE), UP_TILE)
            copy = pltpu.make_async_copy(src.at[:, cols], w_buf.at[slot], w_sem.at[slot])
            copy.start() if start else copy.wait()

        if not start:
            go(w_own, 0)
            return

        @pl.when(at < tiles)
        def _():
            go(w_own, at)

        @pl.when(at >= tiles)
        def _():
            go(w_other, at - tiles)

    def row_copies():
        parts = ((own_ref, 0, 0, own_rows), (x_ref, 1, 0, own_rows), (y_ref, 2, 0, own_rows), (far_a_ref, 3, 0, half), (far_b_ref, 3, half, half))
        for k, (src, flip, shift, size) in enumerate(parts):
            at = pl.multiple_of(jnp.bitwise_xor(chip, flip) * own_rows + shift, half)
            yield pltpu.make_async_copy(src, h_buf.at[pl.ds(at, size), :], h_sem.at[k])

    @pl.when(step == 0)
    def _():
        weight_copy(step, True)
        for copy in row_copies():
            copy.start()

    @pl.when(step + 1 < 2 * tiles)
    def _():
        weight_copy(step + 1, True)

    weight_copy(step, False)

    @pl.when(step == 0)
    def _():
        for copy in row_copies():
            copy.wait()

    slot = lax.rem(step, 2)
    bias = b_ref[...].astype(F32)

    @pl.loop(0, h_buf.shape[0] // UP_ROWS)
    def _(block):
        here = pl.ds(pl.multiple_of(block * UP_ROWS, UP_ROWS), UP_ROWS)
        up = jnp.dot(h_buf[here, :], w_buf[slot], preferred_element_type=F32)
        up = (up + bias).astype(BF16).astype(F32)
        for pair in range(UP_TILE // (2 * GLU_BLOCK)):
            base = 2 * GLU_BLOCK * pair
            value, gate = up[:, base:base + GLU_BLOCK], up[:, base + GLU_BLOCK:base + 2 * GLU_BLOCK]
            m_ref[here, GLU_BLOCK * pair:GLU_BLOCK * (pair + 1)] = (value * jax.nn.gelu(gate, approximate=True)).astype(BF16)


def up_glu(info, row_parts, w_own, w_other, b_all):
    own_rows, depth = row_parts[0].shape
    rows = 4 * own_rows
    width = w_own.shape[1]
    tiles = width // UP_TILE
    hbm = pl.BlockSpec(memory_space=pl.ANY)
    return pl.pallas_call(
        functools.partial(up_kernel, tiles, own_rows),
        out_shape=jax.ShapeDtypeStruct((rows, width), BF16),
        grid_spec=pltpu.PrefetchScalarGridSpec(
            num_scalar_prefetch=1,
            grid=(2 * tiles,),
            in_specs=[hbm] * 7 + [pl.BlockSpec((1, UP_TILE), lambda j, info: (0, j))],
            out_specs=pl.BlockSpec((rows, UP_TILE // 2), lambda j, info: (0, j)),
            scratch_shapes=[
                pltpu.VMEM((rows, depth), BF16),
                pltpu.VMEM((2, depth, UP_TILE), BF16),
                pltpu.SemaphoreType.DMA((5,)),
                pltpu.SemaphoreType.DMA((2,)),
            ],
        ),
        compiler_params=pltpu.CompilerParams(vmem_limit_bytes=VMEM_LIMIT),
        cost_estimate=pl.CostEstimate(flops=4 * rows * depth * width, bytes_accessed=4 * depth * width, transcendentals=rows * width),
        name='up_glu',
    )(info, *row_parts, w_own, w_other, b_all)


def pair_kernel(a_ref, b_ref, wa_ref, wb_ref, out_ref):
    first = jnp.dot(a_ref[...], wa_ref[...], preferred_element_type=F32).astype(BF16)
    second = jnp.dot(b_ref[...], wb_ref[...], preferred_element_type=F32).astype(BF16)
    out_ref[...] = (first.astype(F32) + second.astype(F32)).astype(BF16)


def pair_product(lhs, w_own, w_other, tile, row_tile):
    depth, width = w_own.shape
    rows = lhs[0].shape[0]
    second = 1 if lhs[0] is lhs[1] else 0
    w_spec = pl.BlockSpec((depth, tile), lambda j, i: (0, j))
    return pl.pallas_call(
        pair_kernel,
        out_shape=jax.ShapeDtypeStruct((rows, width), BF16),
        grid=(width // tile, rows // row_tile),
        in_specs=[
            pl.BlockSpec((row_tile, depth), lambda j, i: (i, 0)),
            pl.BlockSpec((row_tile, depth), lambda j, i: (i, second)),
            w_spec,
            w_spec,
        ],
        out_specs=pl.BlockSpec((row_tile, tile), lambda j, i: (i, j)),
        compiler_params=pltpu.CompilerParams(vmem_limit_bytes=VMEM_LIMIT),
        cost_estimate=pl.CostEstimate(flops=4 * rows * depth * width, bytes_accessed=4 * depth * width, transcendentals=0),
    )(*lhs, w_own, w_other)


def solution(mesh):
    tp = mesh.shape['tp']
    same_core = [list(range(0, tp, 2)), list(range(1, tp, 2))]

    def from_peer(val, flip):
        return lax.ppermute(val, 'tp', [(i, i ^ flip) for i in range(tp)])

    def layer(x_loc, positions, prefix_len, w_qkv, b_qkv, w_out, b_out, ln1_gain, ln1_bias, w_up, b_up, w_down, b_down, ln2_gain, ln2_bias):
        batch_size, seq_loc, _ = x_loc.shape
        me = lax.axis_index('tp')
        half = seq_loc // 2
        gathered = [lax.all_gather(x_loc[0], 'tp', axis=0, tiled=True)]
        cos_t, sin_t = rope_tables(positions)
        infos = [jnp.stack([prefix_len[b], me % 2, me // 2]).astype(jnp.int32) for b in range(batch_size)]
        out_other, up_other, down_other = from_peer(w_out, 1), from_peer(w_up, 1), from_peer(w_down, 1)
        b_all = jnp.concatenate([b_up, from_peer(b_up, 1)]).reshape(1, -1)

        def near_rows(rows):
            return from_peer(rows, 2), from_peer(rows, 4)

        def far_rows(near):
            return from_peer(near[1][:half], 2), from_peer(near[0][half:], 4)

        last_row = batch_size - 1
        x_late, cos_t, sin_t = lax.optimization_barrier((x_loc, cos_t, sin_t))
        for b in range(1, last_row):
            gathered.append(lax.all_gather(x_late[b], 'tp', axis=0, tiled=True))
        gathered[0], x_last = lax.optimization_barrier((gathered[0], x_late[last_row]))
        near_x = near_rows(x_last)

        attn_loc = []
        for b in range(batch_size):
            if b < last_row:
                row_refs, pieces = (gathered[b],), (None,)
            else:
                row_refs = (x_last, *near_x, *far_x)
                swapped = tuple(from_peer(r, 1) for r in row_refs)
                swapped, up_other, down_other = lax.optimization_barrier((swapped, up_other, down_other))
                row_refs = (*row_refs, *swapped)
                pieces = tuple((flip, other, shift, size, seq_loc) for other in (0, 1) for flip, shift, size in (
                    (0, 0, seq_loc), (1, 0, seq_loc), (2, 0, seq_loc), (3, 0, half), (3, half, half)))
            qkv = qkv_product(infos[b], row_refs, pieces, w_qkv, b_qkv)
            mine, other = attention(infos[b], qkv, cos_t[b], sin_t[b], seq_loc)
            if b == 0:
                mine, near_x = lax.optimization_barrier((mine, near_x))
                far_x = far_rows(near_x)
            part = pair_product((mine, from_peer(other, 1)), w_out, out_other, 1024, 768)
            attn_loc.append(lax.psum_scatter(part, 'tp', scatter_dimension=0, axis_index_groups=same_core, tiled=True))

        def first_norm(b):
            return norm_rows(x_loc, b, attn_loc[b], b_out, ln1_gain, ln1_bias)

        result = None
        mid = first_norm(0)
        near = near_rows(mid)
        far = far_rows(near)
        for b in range(batch_size):
            parts = (mid, *near, *far)
            last = b == batch_size - 1
            if not last:
                parts, next_mid = lax.optimization_barrier((parts, first_norm(b + 1)))
                next_near = near_rows(next_mid)
            acts = up_glu(infos[b], parts, w_up, up_other, b_all)
            if not last:
                acts, next_near = lax.optimization_barrier((acts, next_near))
                next_far = far_rows(next_near)
            part = pair_product((acts, acts), w_down, down_other, 512, 768)
            ffn_loc = lax.psum_scatter(part, 'tp', scatter_dimension=0, axis_index_groups=same_core, tiled=True)
            result = norm_rows(mid, None, ffn_loc, b_down, ln2_gain, ln2_bias, batch_size, b, result)
            if not last:
                mid, near, far = next_mid, next_near, next_far
        return result

    in_specs = (P('dp', 'tp', None), P('dp', None), P('dp'), P(None, 'tp'), P('tp'), P('tp', None), P(), P(), P(), P(None, 'tp'), P('tp'), P('tp', None), P(), P(), P())
    return jax.shard_map(layer, mesh=mesh, in_specs=in_specs, out_specs=P('dp', 'tp', None), check_vma=False)
```

```python
import functools
import math
import jax
import jax.numpy as jnp
from jax import lax
from jax.experimental import pallas as pl
from jax.experimental.pallas import tpu as pltpu
from jax.sharding import PartitionSpec as P


HEAD_DIM = 128
GLU_BLOCK = 128
DEEPNORM_ALPHA = math.sqrt(2.0 * 70)
LN_EPS = 1e-5
ROPE_BASE = 10000.0
VMEM_LIMIT = 60 << 20
F32 = jnp.float32
BF16 = jnp.bfloat16


def layer_norm(resid, ln_gain, ln_bias):
    mean_val = jnp.mean(resid, axis=-1, keepdims=True)
    centered = resid - mean_val
    var_val = jnp.mean(centered * centered, axis=-1, keepdims=True)
    return centered * lax.rsqrt(var_val + LN_EPS) * ln_gain.astype(F32) + ln_bias.astype(F32)


def rope_tables(positions):
    inv_freq = ROPE_BASE ** (jnp.arange(HEAD_DIM // 2, dtype=F32) * (-2.0 / HEAD_DIM))
    angles = positions.astype(F32)[:, :, None] * inv_freq
    cos_t, sin_t = jnp.cos(angles), jnp.sin(angles)
    return jnp.concatenate([cos_t, cos_t], axis=-1), jnp.concatenate([-sin_t, sin_t], axis=-1)


def rotate(vec, cos_t, sin_t):
    wide = vec.astype(F32)
    return (wide * cos_t + pltpu.roll(wide, HEAD_DIM // 2, 1) * sin_t).astype(BF16)


def attn_kernel(rows, seq_len, key_block, info, qkv_ref, cos_ref, sin_ref, mine_ref, other_ref, k_ref):
    q_blk = pl.program_id(1)
    prefix, core = info[0], info[1]
    q_rows = 2 * rows

    @pl.when(q_blk == 0)
    def _():
        k_ref[...] = rotate(qkv_ref[:, HEAD_DIM:2 * HEAD_DIM], cos_ref[...], sin_ref[...])

    q_start = pl.multiple_of(q_blk * q_rows, q_rows)
    limit = jnp.maximum(prefix, q_start + q_rows)
    need = lax.div(limit + (key_block - 1), key_block)
    exp_scale = HEAD_DIM ** -0.5 * math.log2(math.e)

    def half(which, keys):
        at = pl.multiple_of(q_start + which * rows, rows)
        here = pl.ds(at, rows)
        q_rot = rotate(qkv_ref[here, 0:HEAD_DIM], cos_ref[here, :], sin_ref[here, :])
        scores = lax.dot_general(q_rot, k_ref[0:keys, :], (((1,), (1,)), ((), ())), preferred_element_type=F32)
        row_last = jnp.maximum(lax.broadcasted_iota(jnp.int32, (rows, 1), 0) + at, prefix - 1)
        key_idx = lax.broadcasted_iota(jnp.int32, (rows, keys), 1)
        scores = jnp.where(key_idx <= row_last, scores, -1e30)
        top = jnp.max(scores, axis=-1, keepdims=True)
        probs = jnp.exp2(scores * exp_scale - top * exp_scale)
        inv_sum = 1.0 / jnp.sum(probs, axis=-1, keepdims=True)
        probs = (probs * inv_sum).astype(BF16)
        v_all = qkv_ref[0:keys, 2 * HEAD_DIM:3 * HEAD_DIM]
        return jnp.dot(probs, v_all, preferred_element_type=F32)

    for blocks in range(1, seq_len // key_block + 1):
        @pl.when(need == blocks)
        def _(keys=blocks * key_block):
            first, second = half(0, keys), half(1, keys)
            mine_ref[...] = jnp.where(core == 0, first, second).astype(BF16)
            other_ref[...] = jnp.where(core == 0, second, first).astype(BF16)


def attention(info, qkv, cos_t, sin_t, rows):
    seq_len, width = qkv.shape
    heads = width // (3 * HEAD_DIM)
    half_len = seq_len // 2
    key_block = 2 * rows
    out = jax.ShapeDtypeStruct((half_len, heads * HEAD_DIM), BF16)
    out_spec = pl.BlockSpec((rows, HEAD_DIM), lambda h, i, info: (i, h))
    return pl.pallas_call(
        functools.partial(attn_kernel, rows, seq_len, key_block),
        out_shape=(out, out),
        grid_spec=pltpu.PrefetchScalarGridSpec(
            num_scalar_prefetch=1,
            grid=(heads, seq_len // (2 * rows)),
            in_specs=[
                pl.BlockSpec((seq_len, 3 * HEAD_DIM), lambda h, i, info: (0, h)),
                pl.BlockSpec((seq_len, HEAD_DIM), lambda h, i, info: (0, 0)),
                pl.BlockSpec((seq_len, HEAD_DIM), lambda h, i, info: (0, 0)),
            ],
            out_specs=[out_spec, out_spec],
            scratch_shapes=[pltpu.VMEM((seq_len, HEAD_DIM), BF16)],
        ),
        compiler_params=pltpu.CompilerParams(vmem_limit_bytes=VMEM_LIMIT),
        cost_estimate=pl.CostEstimate(flops=24 * 10 ** 9, bytes_accessed=12 << 20, transcendentals=heads * seq_len * seq_len),
        name='attention',
    )(info, qkv, cos_t, sin_t)


def norm_kernel(x_ref, part_ref, bias_ref, gain_ref, shift_ref, *out_refs):
    resid = DEEPNORM_ALPHA * x_ref[...].astype(F32) + part_ref[...].astype(F32) + bias_ref[...].astype(F32)
    out_refs[-1][...] = layer_norm(resid, gain_ref[...], shift_ref[...]).astype(BF16)


NORM_ROWS = 96


def norm_rows(x_rows, x_at, part, bias, gain, shift, lo=0, out_shape=None, out_at=None, into=None):
    rows, width = part.shape
    skip = lo // NORM_ROWS
    vec = pl.BlockSpec((1, width), lambda i: (0, 0))
    if x_at is None:
        x_spec = pl.BlockSpec((NORM_ROWS, width), lambda i: (skip + i, 0))
    else:
        x_spec = pl.BlockSpec((None, NORM_ROWS, width), lambda i: (x_at, skip + i, 0))
    args = [x_rows, part, bias.reshape(1, -1), gain.reshape(1, -1), shift.reshape(1, -1)]
    in_specs = [x_spec, pl.BlockSpec((NORM_ROWS, width), lambda i: (i, 0)), vec, vec, vec]
    alias = {}
    if out_shape is None:
        out, out_spec = jax.ShapeDtypeStruct((rows, width), BF16), in_specs[1]
    else:
        out = jax.ShapeDtypeStruct(out_shape, BF16)
        out_spec = pl.BlockSpec((None, NORM_ROWS, width), lambda i: (out_at, skip + i, 0))
    if into is not None:
        args.append(into)
        in_specs.append(pl.BlockSpec(memory_space=pl.ANY))
        alias = {5: 0}
    return pl.pallas_call(
        norm_kernel,
        out_shape=out,
        grid=(rows // NORM_ROWS,),
        in_specs=in_specs,
        out_specs=out_spec,
        input_output_aliases=alias,
        compiler_params=pltpu.CompilerParams(vmem_limit_bytes=VMEM_LIMIT),
        cost_estimate=pl.CostEstimate(flops=3 * 10 ** 9, bytes_accessed=6 * rows * width, transcendentals=0),
        name='norm_rows',
    )(*args)


QKV_TILE = 512
ROW_BLOCK = 384


def qkv_kernel(pieces, info, *refs):
    piece_refs, (w_ref, b_ref, out_ref, x_buf, x_sem) = refs[:len(pieces)], refs[len(pieces):]
    first = pl.program_id(0) == 0
    in_order = pieces[0] is None
    bias = b_ref[...].astype(F32)

    def piece_copy(k):
        if in_order:
            return pltpu.make_async_copy(
                piece_refs[0].at[pl.ds(k * ROW_BLOCK, ROW_BLOCK), :], x_buf.at[pl.ds(k * ROW_BLOCK, ROW_BLOCK), :], x_sem.at[k])
        flip, other, shift, size, whole = pieces[k]
        device = 2 * jnp.bitwise_xor(info[2], flip) + jnp.bitwise_xor(info[1], other)
        at = pl.multiple_of(device * whole + shift, size)
        return pltpu.make_async_copy(piece_refs[k], x_buf.at[pl.ds(at, size), :], x_sem.at[k])

    blocks = x_buf.shape[0] // ROW_BLOCK
    copies = blocks if in_order else len(pieces)

    @pl.when(first)
    def _():
        for k in range(copies):
            piece_copy(k).start()
        if not in_order:
            for k in range(copies):
                piece_copy(k).wait()

    @pl.loop(0, blocks)
    def _(block):
        here = pl.ds(pl.multiple_of(block * ROW_BLOCK, ROW_BLOCK), ROW_BLOCK)
        if in_order:
            @pl.when(first)
            def _():
                pltpu.make_async_copy(piece_refs[0].at[here, :], x_buf.at[here, :], x_sem.at[block]).wait()
        out_ref[here, :] = (jnp.dot(x_buf[here, :], w_ref[...], preferred_element_type=F32) + bias).astype(BF16)


def qkv_product(info, row_refs, pieces, w_qkv, b_qkv):
    depth, width = w_qkv.shape
    rows = sum(r.shape[0] for r in row_refs)
    hbm = pl.BlockSpec(memory_space=pl.ANY)
    return pl.pallas_call(
        functools.partial(qkv_kernel, pieces),
        out_shape=jax.ShapeDtypeStruct((rows, width), BF16),
        grid_spec=pltpu.PrefetchScalarGridSpec(
            num_scalar_prefetch=1,
            grid=(width // QKV_TILE,),
            in_specs=[hbm] * len(row_refs) + [
                pl.BlockSpec((depth, QKV_TILE), lambda j, info: (0, j)),
                pl.BlockSpec((1, QKV_TILE), lambda j, info: (0, j)),
            ],
            out_specs=pl.BlockSpec((rows, QKV_TILE), lambda j, info: (0, j)),
            scratch_shapes=[
                pltpu.VMEM((rows, depth), BF16),
                pltpu.SemaphoreType.DMA((max(len(pieces), rows // ROW_BLOCK),)),
            ],
        ),
        compiler_params=pltpu.CompilerParams(vmem_limit_bytes=VMEM_LIMIT),
        cost_estimate=pl.CostEstimate(flops=2 * rows * depth * width, bytes_accessed=2 * depth * (rows + width), transcendentals=0),
        name='qkv',
    )(info, *row_refs, w_qkv, b_qkv.reshape(1, -1))


UP_TILE = 512
UP_ROWS = 384


def up_kernel(tiles, pieces, size, info, *refs):
    piece_refs, (w_own, w_other, b_ref, m_ref, h_buf, w_buf, h_sem, w_sem) = refs[:len(pieces)], refs[len(pieces):]
    step = pl.program_id(0)
    chip = info[2]

    def weight_copy(at, start):
        slot = lax.rem(at, 2)

        def go(src, tile):
            cols = pl.ds(pl.multiple_of(tile * UP_TILE, UP_TILE), UP_TILE)
            copy = pltpu.make_async_copy(src.at[:, cols], w_buf.at[slot], w_sem.at[slot])
            copy.start() if start else copy.wait()

        if not start:
            go(w_own, 0)
            return

        @pl.when(at < tiles)
        def _():
            go(w_own, at)

        @pl.when(at >= tiles)
        def _():
            go(w_other, at - tiles)

    def row_copies():
        for k, (flip, src_at, dst_at, count) in enumerate(pieces):
            at = pl.multiple_of(jnp.bitwise_xor(chip, flip) * size + dst_at, NORM_ROWS)
            yield pltpu.make_async_copy(piece_refs[k].at[pl.ds(src_at, count), :], h_buf.at[pl.ds(at, count), :], h_sem.at[k])

    @pl.when(step == 0)
    def _():
        weight_copy(step, True)
        for copy in row_copies():
            copy.start()

    @pl.when(step + 1 < 2 * tiles)
    def _():
        weight_copy(step + 1, True)

    weight_copy(step, False)

    @pl.when(step == 0)
    def _():
        for copy in row_copies():
            copy.wait()

    slot = lax.rem(step, 2)
    bias = b_ref[...].astype(F32)

    @pl.loop(0, h_buf.shape[0] // UP_ROWS)
    def _(block):
        here = pl.ds(pl.multiple_of(block * UP_ROWS, UP_ROWS), UP_ROWS)
        up = jnp.dot(h_buf[here, :], w_buf[slot], preferred_element_type=F32)
        up = (up + bias).astype(BF16).astype(F32)
        for pair in range(UP_TILE // (2 * GLU_BLOCK)):
            base = 2 * GLU_BLOCK * pair
            value, gate = up[:, base:base + GLU_BLOCK], up[:, base + GLU_BLOCK:base + 2 * GLU_BLOCK]
            m_ref[here, GLU_BLOCK * pair:GLU_BLOCK * (pair + 1)] = (value * jax.nn.gelu(gate, approximate=True)).astype(BF16)


def up_glu(info, row_parts, lo, size, w_own, w_other, b_all):
    own_rows, depth = row_parts[0].shape
    half = own_rows // 2
    refs = list(row_parts[:3])
    pieces = [(flip, lo, 0, size) for flip in range(3)]
    for part in range(2):
        if lo <= part * half < lo + size:
            refs.append(row_parts[3 + part])
            pieces.append((3, 0, part * half - lo, half))
    rows = 4 * size
    width = w_own.shape[1]
    tiles = width // UP_TILE
    hbm = pl.BlockSpec(memory_space=pl.ANY)
    return pl.pallas_call(
        functools.partial(up_kernel, tiles, tuple(pieces), size),
        out_shape=jax.ShapeDtypeStruct((rows, width), BF16),
        grid_spec=pltpu.PrefetchScalarGridSpec(
            num_scalar_prefetch=1,
            grid=(2 * tiles,),
            in_specs=[hbm] * (len(refs) + 2) + [pl.BlockSpec((1, UP_TILE), lambda j, info: (0, j))],
            out_specs=pl.BlockSpec((rows, UP_TILE // 2), lambda j, info: (0, j)),
            scratch_shapes=[
                pltpu.VMEM((rows, depth), BF16),
                pltpu.VMEM((2, depth, UP_TILE), BF16),
                pltpu.SemaphoreType.DMA((len(refs),)),
                pltpu.SemaphoreType.DMA((2,)),
            ],
        ),
        compiler_params=pltpu.CompilerParams(vmem_limit_bytes=VMEM_LIMIT),
        cost_estimate=pl.CostEstimate(flops=4 * rows * depth * width, bytes_accessed=4 * depth * width, transcendentals=rows * width),
        name='up_glu',
    )(info, *refs, w_own, w_other, b_all)


def pair_kernel(a_ref, b_ref, wa_ref, wb_ref, out_ref):
    first = jnp.dot(a_ref[...], wa_ref[...], preferred_element_type=F32).astype(BF16)
    second = jnp.dot(b_ref[...], wb_ref[...], preferred_element_type=F32).astype(BF16)
    out_ref[...] = (first.astype(F32) + second.astype(F32)).astype(BF16)


def pair_product(lhs, w_own, w_other, tile, row_tile):
    depth, width = w_own.shape
    rows = lhs[0].shape[0]
    second = 1 if lhs[0] is lhs[1] else 0
    w_spec = pl.BlockSpec((depth, tile), lambda j, i: (0, j))
    return pl.pallas_call(
        pair_kernel,
        out_shape=jax.ShapeDtypeStruct((rows, width), BF16),
        grid=(width // tile, rows // row_tile),
        in_specs=[
            pl.BlockSpec((row_tile, depth), lambda j, i: (i, 0)),
            pl.BlockSpec((row_tile, depth), lambda j, i: (i, second)),
            w_spec,
            w_spec,
        ],
        out_specs=pl.BlockSpec((row_tile, tile), lambda j, i: (i, j)),
        compiler_params=pltpu.CompilerParams(vmem_limit_bytes=VMEM_LIMIT),
        cost_estimate=pl.CostEstimate(flops=4 * rows * depth * width, bytes_accessed=4 * depth * width, transcendentals=0),
    )(*lhs, w_own, w_other)


def solution(mesh):
    tp = mesh.shape['tp']
    same_core = [list(range(0, tp, 2)), list(range(1, tp, 2))]

    def from_peer(val, flip):
        return lax.ppermute(val, 'tp', [(i, i ^ flip) for i in range(tp)])

    def layer(x_loc, positions, prefix_len, w_qkv, b_qkv, w_out, b_out, ln1_gain, ln1_bias, w_up, b_up, w_down, b_down, ln2_gain, ln2_bias):
        batch_size, seq_loc, _ = x_loc.shape
        me = lax.axis_index('tp')
        half = seq_loc // 2
        gathered = [lax.all_gather(x_loc[0], 'tp', axis=0, tiled=True)]
        cos_t, sin_t = rope_tables(positions)
        infos = [jnp.stack([prefix_len[b], me % 2, me // 2]).astype(jnp.int32) for b in range(batch_size)]
        out_other, up_other, down_other = from_peer(w_out, 1), from_peer(w_up, 1), from_peer(w_down, 1)
        b_all = jnp.concatenate([b_up, from_peer(b_up, 1)]).reshape(1, -1)

        def near_rows(rows):
            return from_peer(rows, 2), from_peer(rows, 4)

        def far_rows(near):
            return from_peer(near[1][:half], 2), from_peer(near[0][half:], 4)

        last_row = batch_size - 1
        x_late, cos_t, sin_t = lax.optimization_barrier((x_loc, cos_t, sin_t))
        for b in range(1, last_row):
            gathered.append(lax.all_gather(x_late[b], 'tp', axis=0, tiled=True))
        gathered[0], x_last = lax.optimization_barrier((gathered[0], x_late[last_row]))
        near_x = near_rows(x_last)

        def first_norm(b):
            return norm_rows(x_loc, b, attn_loc[b], b_out, ln1_gain, ln1_bias)

        attn_loc = []
        for b in range(batch_size):
            if b < last_row:
                row_refs, pieces = (gathered[b],), (None,)
            else:
                row_refs = (x_last, *near_x, *far_x)
                swapped = tuple(from_peer(r, 1) for r in row_refs)
                mid = first_norm(0)
                swapped, up_other, down_other, mid = lax.optimization_barrier((swapped, up_other, down_other, mid))
                near = near_rows(mid)
                row_refs = (*row_refs, *swapped)
                pieces = tuple((flip, other, shift, size, seq_loc) for other in (0, 1) for flip, shift, size in (
                    (0, 0, seq_loc), (1, 0, seq_loc), (2, 0, seq_loc), (3, 0, half), (3, half, half)))
            qkv = qkv_product(infos[b], row_refs, pieces, w_qkv, b_qkv)
            mine, other = attention(infos[b], qkv, cos_t[b], sin_t[b], seq_loc)
            if b == 0:
                mine, near_x = lax.optimization_barrier((mine, near_x))
                far_x = far_rows(near_x)
            if b == last_row:
                mine, near = lax.optimization_barrier((mine, near))
                far = far_rows(near)
            part = pair_product((mine, from_peer(other, 1)), w_out, out_other, 1024, 768)
            attn_loc.append(lax.psum_scatter(part, 'tp', scatter_dimension=0, axis_index_groups=same_core, tiled=True))

        result = None
        for b in range(batch_size):
            parts = (mid, *near, *far)
            last = b == last_row
            if not last:
                parts, next_mid = lax.optimization_barrier((parts, first_norm(b + 1)))
                next_near = near_rows(next_mid)
            size = half if last else seq_loc
            for lo in range(0, seq_loc, size):
                acts = up_glu(infos[b], parts, lo, size, w_up, up_other, b_all)
                if not last:
                    acts, next_near = lax.optimization_barrier((acts, next_near))
                    next_far = far_rows(next_near)
                part = pair_product((acts, acts), w_down, down_other, 512, 4 * size)
                ffn_loc = lax.psum_scatter(part, 'tp', scatter_dimension=0, axis_index_groups=same_core, tiled=True)
                result = norm_rows(mid, None, ffn_loc, b_down, ln2_gain, ln2_bias, lo, x_loc.shape, b, result)
            if not last:
                mid, near, far = next_mid, next_near, next_far
        return result

    in_specs = (P('dp', 'tp', None), P('dp', None), P('dp'), P(None, 'tp'), P('tp'), P('tp', None), P(), P(), P(), P(None, 'tp'), P('tp'), P('tp', None), P(), P(), P())
    return jax.shard_map(layer, mesh=mesh, in_specs=in_specs, out_specs=P('dp', 'tp', None), check_vma=False)
```
